32 devices in a mesh: face: 16 (over z, y, core), sub: 2 (over x).
Axes of the slice: x: 2, y: 2, z: 4, core: 2. Of those that a mesh axis runs over, the one named last changes fastest.
Arguments:
- prognostic: bfloat16 [3, 2048, 16, 128], P(None, ('face', 'sub')), may hold values from -4 to 4
- metric: float32 [4, 2048, 16], P(None, ('face', 'sub')), may hold values from -0.35 to 1.6, as said below
- coriolis: float32 [2048, 16], P(('face', 'sub')), may hold values from -1.5 to 1.5
- node_point: int32 [2048, 16], P(('face', 'sub')), may hold values from 0 to 678, as said below
- send_point: int32 [6784], P(('face', 'sub')), may hold values from 0 to 678, as said below
- recv_point: int32 [6784], P(('face', 'sub')), may hold values from 0 to 678, as said below
Outputs:
- advanced: bfloat16 [3, 2048, 16, 128], P(None, ('face', 'sub'))
The draws below stay inside these ranges and needn't reach their ends.
Inputs may be any that keep to these rules, and one draw needn't show every extreme that they name: `node_point`: each device's numbers are its 679 local points; element nodes that are the same point of the surface on one device carry the same number. `send_point`: on every device the 212 slots form groups in this order: 7 slots of offset +1, 7 of offset -1, 97 of offset +8, 97 of offset -8, then one slot each of offsets 8 + 1, -8 - 1, 7, 1 - 8. A slot names the sender's point that the device at curve index d + o, taken modulo 32, shares. Every slot is used. `recv_point`: slot s of device d names the local point that is the same surface point as the sender's slot s, the sender being the device at d minus the slot's group offset modulo 32. The copies of every shared point are linked between every two devices that hold them. `metric`: entries 0 and 3 lie in [0.6, 1.6], entries 1 and 2 in [-0.35, 0.35].
All inputs are finite; a program needn't handle non-finite values.
Results may differ from the reference program's by a relative error of at most 0.007.
Values sent between devices are 32-bit elements; how exact they have to be, the bound alone decides.
A program may use at most 64 MiB of HBM per device.

```python
import math
import jax
import jax.numpy as jnp
import numpy as np
from jax import lax

BX = 32
BY = 2
LEV = 128
ELEMS = 64
BLOCKS = 32
ELEMENTS = 2048
LAP = 8
PTS = 679
LINKS = 212


def link_grid_points():
    grid_width = 3 * BX + 1
    grid_height = 3 * BY + 1
    sender = []
    receiver = []
    for height in range(grid_height):
        sender.append(height * grid_width + 3 * BX)
        receiver.append(height * grid_width)
    for height in range(grid_height):
        sender.append(height * grid_width)
        receiver.append(height * grid_width + 3 * BX)
    for column in range(grid_width):
        sender.append(3 * BY * grid_width + column)
        receiver.append(column)
    for column in range(grid_width):
        sender.append(column)
        receiver.append(3 * BY * grid_width + column)
    sender.append(3 * BY * grid_width + 3 * BX)
    receiver.append(0)
    sender.append(0)
    receiver.append(3 * BY * grid_width + 3 * BX)
    sender.append(3 * BY * grid_width)
    receiver.append(3 * BX)
    sender.append(3 * BX)
    receiver.append(3 * BY * grid_width)
    return (np.array(sender, np.int32), np.array(receiver, np.int32))


def mesh_tables(key):
    base = jax.random.fold_in(key, 4242)
    key_elem, key_rot, key_point = jax.random.split(base, 3)
    elements = BX * BY
    placement_order = jax.vmap(lambda sub_key: jax.random.permutation(sub_key, elements))(jax.random.split(key_elem, BLOCKS)).astype(jnp.int32)
    rotation = jax.random.randint(key_rot, (BLOCKS, elements), 0, 4).astype(jnp.int32)[..., None]
    relabel = jax.vmap(lambda sub_key: jax.random.permutation(sub_key, PTS))(jax.random.split(key_point, BLOCKS)).astype(jnp.int32)
    across = placement_order % BX
    upward = placement_order // BX
    node_index = jnp.arange(16, dtype=jnp.int32)
    node_row = node_index // 4
    node_col = node_index % 4
    rot_col = jnp.where(rotation == 0, node_col, jnp.where(rotation == 1, 3 - node_row, jnp.where(rotation == 2, 3 - node_col, node_row)))
    rot_row = jnp.where(rotation == 0, node_row, jnp.where(rotation == 1, node_col, jnp.where(rotation == 2, 3 - node_row, 3 - node_col)))
    grid_index = (3 * upward[..., None] + rot_row) * (3 * BX + 1) + 3 * across[..., None] + rot_col
    node_table = jnp.take_along_axis(relabel, grid_index.reshape(BLOCKS, elements * 16).astype(jnp.int32), axis=1)
    sender, receiver = link_grid_points()
    send_table = relabel[:, jnp.asarray(sender)].reshape(-1).astype(jnp.int32)
    recv_table = relabel[:, jnp.asarray(receiver)].reshape(-1).astype(jnp.int32)
    return (node_table.reshape(ELEMENTS, 16).astype(jnp.int32), send_table, recv_table)


def draw_node_point(key, part):
    return mesh_tables(key)[0]


def draw_send_point(key, part):
    return mesh_tables(key)[1]


def draw_recv_point(key, part):
    return mesh_tables(key)[2]


def draw_metric(key, part):
    key_diag, key_off = jax.random.split(jax.random.fold_in(key, 17), 2)
    diagonal = jnp.exp(jax.random.uniform(key_diag, (2, ELEMENTS, 16), jnp.float32, math.log(0.6), math.log(1.6)))
    off_diag = jax.random.uniform(key_off, (2, ELEMENTS, 16), jnp.float32, -0.35, 0.35)
    diagonal = jnp.clip(diagonal, 0.6, 1.6)
    return jnp.stack([diagonal[0], off_diag[0], off_diag[1], diagonal[1]]).astype(jnp.float32)


def block_levels(own_key, shape, cuts, least, high):
    level, own = 1.0, jax.random.fold_in(own_key, 6)
    for position, parts in cuts:
        heights = jnp.exp(jax.random.uniform(jax.random.fold_in(own, position), (parts,), jnp.float32, least / len(cuts), high / len(cuts)))
        level = level * jnp.repeat(heights, shape[position] // parts).reshape([-1 if axis == position else 1 for axis in range(len(shape))])
    return level


def gaussian(own_key, dims, spread, most, cuts=(), held_as=jnp.bfloat16):
    loudness = block_levels(own_key, dims, cuts, -0.22, 0.18) if cuts else 1.0
    values = jax.random.normal(own_key, dims, jnp.float32) * spread * loudness
    return jnp.minimum(jnp.maximum(values, -most), most).astype(held_as)


def setup_inputs(seed: int = 0) -> dict:
    streams_of = jax.random.split(jax.random.key(seed), 7)
    prognostic = gaussian(streams_of[0], (3, ELEMENTS, 16, LEV), 1.0, 4.0, ((1, 32),))
    metric = draw_metric(jax.random.fold_in(streams_of[6], 71), 0)
    coriolis = jnp.clip(jax.random.uniform(streams_of[2], (ELEMENTS, 16), jnp.float32, -1.5, 1.5) * block_levels(streams_of[2], (ELEMENTS, 16), ((0, 32),), -0.4, 0.0), -1.5, 1.5)
    node_point = draw_node_point(jax.random.fold_in(streams_of[6], 71), 0)
    send_point = draw_send_point(jax.random.fold_in(streams_of[6], 71), 0)
    recv_point = draw_recv_point(jax.random.fold_in(streams_of[6], 71), 0)
    return dict(prognostic=prognostic, metric=metric, coriolis=coriolis, node_point=node_point, send_point=send_point, recv_point=recv_point)


STEP_SIZE = 0.1

def gll_tables():
    abscissa = np.array([-1.0, -math.sqrt(0.2), math.sqrt(0.2), 1.0])
    legendre = 0.5 * (5.0 * abscissa * abscissa * abscissa - 3.0 * abscissa)
    derivative = np.zeros((4, 4))
    for target in range(4):
        for source in range(4):
            if target != source:
                derivative[target, source] = legendre[target] / (legendre[source] * (abscissa[target] - abscissa[source]))
    derivative[0, 0] = -3.0
    derivative[3, 3] = 3.0
    weights = np.array([1.0, 5.0, 5.0, 1.0]) / 6.0
    return (derivative, weights)

def along_cols(values, derivative):
    return jnp.einsum('aj,erjl->eral', derivative, values, precision=lax.Precision.HIGHEST)

def along_rows(values, derivative):
    return jnp.einsum('aj,ejcl->eacl', derivative, values, precision=lax.Precision.HIGHEST)

def element_tendency(fields, metric, coriolis):
    elements = fields.shape[1]
    levels = fields.shape[3]
    deriv_table, weight_table = gll_tables()
    derivative = jnp.asarray(deriv_table, dtype=jnp.float32)
    weights = jnp.asarray(weight_table, dtype=jnp.float32)
    shaped = fields.reshape(3, elements, 4, 4, levels)
    veloc_one = shaped[0]
    veloc_two = shaped[1]
    geopot = shaped[2]
    inverse = metric.reshape(4, elements, 4, 4, 1)
    inv_aa = inverse[0]
    inv_ab = inverse[1]
    inv_ba = inverse[2]
    inv_bb = inverse[3]
    jacobian_inv = inv_aa * inv_bb - inv_ab * inv_ba
    energy = 0.5 * (veloc_one * veloc_one + veloc_two * veloc_two) + geopot
    ref_one = along_cols(energy, derivative)
    ref_two = along_rows(energy, derivative)
    grad_one = inv_aa * ref_one + inv_ba * ref_two
    grad_two = inv_ab * ref_one + inv_bb * ref_two
    cov_one = (inv_bb * veloc_one - inv_ba * veloc_two) / jacobian_inv
    cov_two = (inv_aa * veloc_two - inv_ab * veloc_one) / jacobian_inv
    vorticity = jacobian_inv * (along_cols(cov_two, derivative) - along_rows(cov_one, derivative))
    absolute = vorticity + coriolis.reshape(elements, 4, 4, 1)
    flux_one = geopot * veloc_one
    flux_two = geopot * veloc_two
    contra_one = (inv_aa * flux_one + inv_ab * flux_two) / jacobian_inv
    contra_two = (inv_ba * flux_one + inv_bb * flux_two) / jacobian_inv
    divergence = jacobian_inv * (along_cols(contra_one, derivative) + along_rows(contra_two, derivative))
    tendency = jnp.stack([absolute * veloc_two - grad_one, -absolute * veloc_one - grad_two, -divergence])
    mass_weight = (weights[:, None] * weights[None, :])[None] / jacobian_inv[..., 0]
    return (tendency.reshape(3, elements, 16, levels), mass_weight.reshape(elements, 16))

def link_groups(lap_blocks):
    side_points = 3 * BY + 1
    top_points = 3 * BX + 1
    group_sizes = [(1, side_points), (-1, side_points), (lap_blocks, top_points), (-lap_blocks, top_points), (lap_blocks + 1, 1), (-lap_blocks - 1, 1), (lap_blocks - 1, 1), (1 - lap_blocks, 1)]
    groups = []
    first_slot = 0
    for offset, slot_count in group_sizes:
        groups.append((offset, first_slot, slot_count))
        first_slot = first_slot + slot_count
    return groups

def block_terms(prognostic, metric, coriolis, node_point, device_index):
    first_elem = (device_index * ELEMS).astype(jnp.int32)
    fields = lax.dynamic_slice_in_dim(prognostic, first_elem, ELEMS, 1).astype(jnp.float32)
    local_metric = lax.dynamic_slice_in_dim(metric, first_elem, ELEMS, 1)
    local_coriolis = lax.dynamic_slice_in_dim(coriolis, first_elem, ELEMS, 0)
    point_ids = lax.dynamic_slice_in_dim(node_point, first_elem, ELEMS, 0).reshape(-1)
    tendency, mass_weight = element_tendency(fields, local_metric, local_coriolis)
    weighted = (tendency * mass_weight[None, :, :, None]).reshape(3, ELEMS * 16, LEV)
    partial_value = jnp.zeros((3, PTS, LEV), jnp.float32).at[:, point_ids, :].add(weighted)
    weight = jnp.zeros((PTS,), jnp.float32).at[point_ids].add(mass_weight.reshape(-1))
    return (fields, point_ids, partial_value, weight)

def reference(prognostic, metric, coriolis, node_point, send_point, recv_point):
    device_list = jnp.arange(BLOCKS, dtype=jnp.int32)

    def outgoing_of(device_index):
        fields, point_ids, partial_value, weight = block_terms(prognostic, metric, coriolis, node_point, device_index)
        link_ids = lax.dynamic_slice_in_dim(send_point, (device_index * LINKS).astype(jnp.int32), LINKS, 0)
        return (partial_value[:, link_ids, :], weight[link_ids])
    sent_values, sent_weight = lax.map(outgoing_of, device_list)
    groups = link_groups(LAP)

    def advance(device_index, collected):
        fields, point_ids, partial_value, weight = block_terms(prognostic, metric, coriolis, node_point, device_index)
        link_ids = lax.dynamic_slice_in_dim(recv_point, (device_index * LINKS).astype(jnp.int32), LINKS, 0)
        arrived_values = []
        arrived_weight = []
        for offset, first_slot, slot_count in groups:
            source = jnp.mod(device_index - offset, BLOCKS).astype(jnp.int32)
            values_from = lax.dynamic_index_in_dim(sent_values, source, 0, keepdims=False)
            weight_from = lax.dynamic_index_in_dim(sent_weight, source, 0, keepdims=False)
            arrived_values.append(values_from[:, first_slot:first_slot + slot_count, :])
            arrived_weight.append(weight_from[first_slot:first_slot + slot_count])
        total = partial_value.at[:, link_ids, :].add(jnp.concatenate(arrived_values, axis=1))
        total_weight = weight.at[link_ids].add(jnp.concatenate(arrived_weight, axis=0))
        averaged = total[:, point_ids, :] / total_weight[point_ids][None, :, None]
        advanced = (fields + STEP_SIZE * averaged.reshape(3, ELEMS, 16, LEV)).astype(jnp.bfloat16)
        first_elem = (device_index * ELEMS).astype(jnp.int32)
        return lax.dynamic_update_slice_in_dim(collected, advanced, first_elem, 1)
    result = jnp.zeros((3, ELEMENTS, 16, LEV), jnp.bfloat16)
    return lax.fori_loop(0, BLOCKS, advance, result)
```

```python
import functools
import math

import jax
import jax.numpy as jnp
import numpy as np
from jax import lax
from jax.experimental import pallas as pl
from jax.experimental.pallas import tpu as pltpu
from jax.sharding import PartitionSpec as P

BX = 32
BY = 2
STEP_SIZE = 0.1
ROWS = 256
BAND = 128
LANES = 128
BULK = (2, 3)
SMALL = (0, 1, 4, 5, 6, 7)
F32 = jnp.float32
BF16 = jnp.bfloat16
MESH = pl.DeviceIdType.MESH


def gll_tables():
    abscissa = np.array([-1.0, -math.sqrt(0.2), math.sqrt(0.2), 1.0])
    legendre = 0.5 * (5.0 * abscissa * abscissa * abscissa - 3.0 * abscissa)
    derivative = np.zeros((4, 4))
    for target in range(4):
        for source in range(4):
            if target != source:
                derivative[target, source] = legendre[target] / (
                    legendre[source] * (abscissa[target] - abscissa[source])
                )
    derivative[0, 0] = -3.0
    derivative[3, 3] = 3.0
    weights = np.array([1.0, 5.0, 5.0, 1.0]) / 6.0
    return (derivative, weights)


def round_bf16(values):
    return np.asarray(values, dtype=jnp.bfloat16).astype(np.float64)


def operator_tables():
    derivative, weights = gll_tables()
    eye4 = np.eye(4)
    node_weight = np.kron(weights, weights)
    along_c = node_weight[:, None] * np.kron(eye4, derivative)
    along_r = node_weight[:, None] * np.kron(derivative, eye4)
    best = None
    for trial in np.linspace(1.0, 2.0, 2001)[:-1]:
        error = max(
            np.max(np.abs(round_bf16(trial * t) / trial - t) / (np.abs(t).max(1, keepdims=True)))
            for t in (along_c, along_r)
        )
        if best is None or error < best[0]:
            best = (error, trial)
    scale = float(best[1])
    tiles = [np.tile(t, (1, BAND // 16)) for t in (along_c, along_r)]
    stacked = np.concatenate(tiles, axis=0) * scale
    return np.asarray(stacked, dtype=np.float32), scale


def link_groups(lap_blocks):
    side_points = 3 * BY + 1
    top_points = 3 * BX + 1
    group_sizes = [
        (1, side_points),
        (-1, side_points),
        (lap_blocks, top_points),
        (-lap_blocks, top_points),
        (lap_blocks + 1, 1),
        (-lap_blocks - 1, 1),
        (lap_blocks - 1, 1),
        (1 - lap_blocks, 1),
    ]
    starts = [0]
    for _, slot_count in group_sizes:
        starts.append(starts[-1] + slot_count)
    groups = [None] * len(group_sizes)
    first_row = 0
    for k in (0, 1, 2, 4, 3, 5, 6, 7):
        offset, slot_count = group_sizes[k]
        padded = -(-(slot_count + 1) // 8) * 8
        groups[k] = (offset, starts[k], slot_count, first_row, padded)
        first_row += padded
    return groups, first_row


def iota(shape, dim):
    return lax.broadcasted_iota(jnp.int32, shape, dim)


def dot(a, b):
    return lax.dot_general(a, b, (((1,), (0,)), ((), ())), preferred_element_type=F32)


def dot_nt(a, b):
    return lax.dot_general(a, b, (((1,), (1,)), ((), ())), preferred_element_type=F32)


def wait_bytes(ref, sem):
    pltpu.make_async_copy(ref, ref, sem).wait()


def kernel(
    sizes, groups, slots, scale,
    prog_hbm, metric_hbm, cor_hbm, node_hbm, send_hbm, recv_hbm, ops_hbm,
    out_hbm,
    prog, metric, cor, node, sendp, recvp, ops,
    wide, weighted, summed, inverse, table_s, table_r,
    expand, pick, spread, vort, slim,
    outgoing, arrived, in_sem, send_sem, recv_sem, ready, mark,
):
    nface, nsub = sizes
    total = nface * nsub
    nodes = prog.shape[1]
    blocks = nodes // ROWS
    elements = node.shape[1]

    def load(src, dst, k):
        copy = pltpu.make_async_copy(src, dst, in_sem.at[k])
        copy.start()
        return copy

    loads = [load(src, dst, k) for k, (src, dst) in enumerate((
        (metric_hbm, metric), (cor_hbm, cor), (node_hbm, node),
        (send_hbm, sendp), (recv_hbm, recvp), (ops_hbm, ops)))]
    fields = [load(prog_hbm.at[f], prog.at[f], len(loads) + f) for f in range(3)]

    pl.semaphore_signal(mark, 1)
    me = lax.axis_index("face") * nsub + lax.axis_index("sub")
    lap = 4 * nsub

    def rank(index):
        hops = 4 * (index // lap) + lax.rem(index, lap) // (2 * nsub) + lax.rem(index, nsub)
        return hops * total + index

    peers, lower, first_lap = [], [], []
    for offset, *_ in groups:
        other = lax.rem(me + (offset % total), total)
        peers.append((other // nsub, lax.rem(other, nsub)))
        lower.append(rank(other) < rank(me))
        first_lap.append(other < lap)
    higher = [jnp.logical_not(flag) for flag in lower]
    middle = lower[3] & higher[2]

    barrier = pltpu.get_barrier_semaphore()
    for k, peer in enumerate(peers):
        @pl.when(higher[k])
        def _(peer=peer):
            pl.semaphore_signal(barrier, inc=1, device_id=peer, device_id_type=MESH)
    for k, (_, _, used, first_row, padded) in enumerate(groups):
        if k in BULK:
            gap = pl.ds(first_row + used, padded - used)
            arrived[0:2, gap] = jnp.zeros((2, padded - used, arrived.shape[2]), F32)
        if padded > used + 1:
            gap = pl.ds(first_row + used + 1, padded - used - 1)
            part = slice(2, 3) if k in BULK else slice(0, 3)
            arrived[part, gap] = jnp.zeros((part.stop - part.start, padded - used - 1, arrived.shape[2]), F32)

    expand[...] = jnp.where(
        iota((elements, nodes), 0) == iota((elements, nodes), 1) >> 4, 1.0, 0.0).astype(BF16)
    pick_l = (iota((LANES, 3 * LANES), 0) & (LANES // 2 - 1)) >> 4
    pick[...] = jnp.where(pick_l == (iota((LANES, 3 * LANES), 1) >> 7), 1.0, 0.0).astype(BF16)
    for copy in loads:
        copy.wait()

    a, b, e, g = metric[0], metric[1], metric[2], metric[3]
    inv_det = 1.0 / (a * g - b * e)
    lane16 = iota((16, 1), 0)
    col, row = lane16 & 3, lane16 >> 2
    w_node = jnp.where((col == 0) | (col == 3), 1 / 6, 5 / 6) * jnp.where((row == 0) | (row == 3), 1 / 6, 5 / 6)
    mass = w_node * inv_det
    parts = [a * inv_det, b * inv_det, e * inv_det, g * inv_det, node[...].astype(F32)]
    stack = jnp.concatenate(parts, axis=0)
    upper = stack.astype(BF16)
    rest = (stack - upper.astype(F32)).astype(BF16)
    spans = dot(jnp.concatenate([upper, rest], axis=0), expand[...])
    half = stack.shape[0]
    spans = spans[:half] + spans[half:]
    own_row = (iota((16, nodes), 1) & 15) == iota((16, nodes), 0)
    row_a, row_b, row_e, row_g, point_row = [
        jnp.sum(jnp.where(own_row, spans[16 * k:16 * k + 16], 0.0), axis=0, keepdims=True) for k in range(5)]

    stack = jnp.concatenate([scale * (mass * cor[...]), mass, parts[4], jnp.zeros_like(mass)], axis=0)
    upper = stack.astype(BF16).astype(F32)
    both = jnp.concatenate([upper, stack - upper], axis=0).T
    own = (iota((16, LANES), 1) & 15) == iota((16, LANES), 0)
    spread[...] = jnp.where(
        own[None], jnp.broadcast_to(both[:, None, :], (elements, 16, LANES)), 0.0
    ).reshape(nodes, LANES).astype(BF16)

    def tile_rows(table):
        return jnp.concatenate([table] * (nodes // BAND), axis=1)

    along_c = tile_rows(ops[0:16, :].astype(F32))
    along_r = tile_rows(ops[16:32, :].astype(F32))
    slim[0:16, :] = (along_c * row_a + along_r * row_e).astype(BF16)
    slim[16:32, :] = (along_c * row_b + along_r * row_g).astype(BF16)
    slim[32:48, :] = (along_c * spans[0:16] + along_r * spans[32:48]).astype(BF16)
    slim[48:64, :] = (along_c * spans[16:32] + along_r * spans[48:64]).astype(BF16)

    count = sendp.shape[1]
    padded = iota((slots, 1), 0)
    slot_of = jnp.full((slots, 1), -1, jnp.int32)
    for _, first_slot, slot_count, first_row, _ in groups:
        inside = (padded >= first_row) & (padded < first_row + slot_count)
        slot_of = jnp.where(inside, padded - first_row + first_slot, slot_of)
    chosen = slot_of == iota((slots, count), 1)
    vacant = jnp.where(slot_of < 0, -1.0, 0.0)
    send_col = jnp.sum(jnp.where(chosen, sendp[...].astype(F32), 0.0), axis=1, keepdims=True) + vacant
    sign = jnp.where(iota((1, nodes), 1) < nodes // 2, 1.0, -1.0)
    table_s[...] = jnp.where(send_col == point_row, sign, 0.0).astype(BF16)

    for part in range(2):
        rows = pl.ds(part * (nodes // 2), nodes // 2)
        first = dot(spread[rows], pick[:, :2 * LANES])
        wide[0, rows] = first[:, :LANES]
        weighted[3, rows] = first[:, LANES:].astype(BF16)

    for copy in fields:
        copy.wait()

    diagonal = jnp.where(iota((BAND, BAND), 0) >> 4 == iota((BAND, BAND), 1) >> 4, 1.0, 0.0).astype(BF16)

    def block(k, here):
        return jnp.concatenate([slim[k:k + 16, here]] * (BAND // 16), axis=0) * diagonal

    for band in range(nodes // BAND):
        rows = pl.ds(band * BAND, BAND)
        here = pl.ds(band * BAND, BAND)
        left = jnp.concatenate([block(k, here) for k in (0, 16)], axis=1)
        u1, u2, phi = prog[0, rows], prog[1, rows], prog[2, rows]
        right = jnp.concatenate([
            jnp.concatenate([u2, phi * u1], axis=1), jnp.concatenate([-u1, phi * u2], axis=1)], axis=0)
        both_terms = dot(left, right)
        vort[rows, :] = both_terms[:, :LANES]
        weighted[2, rows] = (-both_terms[:, LANES:]).astype(BF16)

    def slot_sum(one, two):
        half = nodes // 2
        terms = [
            dot(table_s[:, h * half:(h + 1) * half],
                jnp.concatenate([weighted[one, pl.ds(h * half, half)], weighted[two, pl.ds(h * half, half)]], axis=1))
            for h in range(2)]
        both_fields = terms[0] - terms[1]
        return both_fields[:, :LANES], both_fields[:, LANES:]

    def copy(k, part, extra, sem):
        rows = pl.ds(groups[k][3], groups[k][2] + extra)
        return pltpu.make_async_remote_copy(
            src_ref=outgoing.at[part, rows], dst_ref=arrived.at[part, rows],
            send_sem=send_sem.at[sem], recv_sem=recv_sem.at[sem],
            device_id=peers[k], device_id_type=MESH)

    def one_field(k):
        return copy(k, pl.ds(2, 1), 1, 0)

    def two_fields(k):
        return copy(k, pl.ds(0, 2), 0, 1)

    def all_fields(k):
        return copy(k, pl.ds(0, 3), 1, 2 + SMALL.index(k))

    def early(copies, flag):
        @pl.when(flag)
        def _():
            for item in copies:
                item.start()

    def late(copies, k):
        @pl.when(higher[k])
        def _():
            pl.semaphore_wait(ready.at[k], 1)
            for item in copies:
                item.start()

    near_two, slot_mass = slot_sum(2, 3)
    outgoing[2] = near_two
    place = jnp.where(iota((slots, LANES), 1) == (iota((slots, LANES), 0) & (LANES - 1)), slot_mass, 0.0)
    for _, _, used, first_row, size in groups:
        outgoing[2, first_row + used:first_row + used + 1] = jnp.sum(
            place[first_row:first_row + size], axis=0, keepdims=True)
    waited = sum(flag.astype(jnp.int32) for flag in lower)

    @pl.when(waited > 0)
    def _():
        pl.semaphore_wait(barrier, waited)

    early([one_field(2)], lower[2])
    early([one_field(3)], middle)
    for k, peer in enumerate(peers):
        @pl.when(lower[k])
        def _(k=k, peer=peer):
            pl.semaphore_signal(ready.at[k ^ 1], inc=1, device_id=peer, device_id_type=MESH)

    for band in range(nodes // BAND):
        rows = pl.ds(band * BAND, BAND)
        here = pl.ds(band * BAND, BAND)
        u1, u2, phi = [prog[f, rows].astype(F32) for f in range(3)]
        energy = (0.5 * (u1 * u1 + u2 * u2) + phi).astype(BF16)
        slopes = dot(jnp.concatenate([block(k, here) for k in (32, 48)], axis=0), energy)
        eta = vort[rows, :] + wide[0, rows]
        weighted[0, rows] = (eta * u2 - slopes[:BAND]).astype(BF16)
        weighted[1, rows] = (-(eta * u1) - slopes[BAND:]).astype(BF16)
    near_zero, near_one = slot_sum(0, 1)
    outgoing[0] = near_zero
    outgoing[1] = near_one
    for k in SMALL:
        early([all_fields(k)], lower[k])
    early([two_fields(2)], lower[2])
    early([two_fields(3)], first_lap[3] & lower[3])
    early([one_field(3), two_fields(3)], lower[3] & lower[2])
    late([one_field(2)], 2)
    for k in (0, 6, 4):
        late([all_fields(k)], k)
    early([two_fields(2)], higher[2])

    recv_col = jnp.sum(jnp.where(chosen, recvp[...].astype(F32), 0.0), axis=1, keepdims=True) + vacant
    same = iota((slots, slots), 0) == iota((slots, slots), 1)
    recv_row = jnp.sum(jnp.where(same, recv_col, 0.0), axis=0, keepdims=True)
    wide[1] = dot(spread[...], pick[:, 2 * LANES:])
    all_weighted = jnp.concatenate([weighted[f] for f in range(4)], axis=1)
    for block in range(blocks):
        rows = pl.ds(block * ROWS, ROWS)
        point = wide[1, rows][:, 0:1]
        meet = jnp.where(point == point_row, 1.0, 0.0).astype(BF16)
        summed[rows, :] = dot(meet, all_weighted)

    early([two_fields(3)], middle & jnp.logical_not(first_lap[3]))
    for k in (1, 5, 7, 3):
        late([one_field(k), two_fields(k)] if k in BULK else [all_fields(k)], k)

    def landing(ref, sem):
        rows_one = sum(groups[k][2] + 1 for k in BULK)
        wait_bytes([
            ref.at[pl.ds(2, 1), pl.ds(0, rows_one)],
            ref.at[pl.ds(0, 2), pl.ds(0, rows_one - 2)],
            *(ref.at[pl.ds(0, 3), pl.ds(0, groups[k][2] + 1)] for k in SMALL),
        ][sem], (send_sem if ref is outgoing else recv_sem).at[sem])

    landing(arrived, 0)
    for k in (5, 7, 1, 6, 4, 0):
        landing(arrived, 2 + SMALL.index(k))
    sides = [jnp.zeros((1, LANES), F32)] * (slots // LANES)
    for _, _, used, first_row, _ in groups:
        sides[first_row // LANES] += arrived[2, first_row + used:first_row + used + 1]
    mass_in = jnp.concatenate(sides, axis=1)
    ones = jnp.ones((slots, LANES), BF16)
    for block in range(blocks):
        rows = pl.ds(block * ROWS, ROWS)
        point = wide[1, rows][:, 0:1]
        hit = point == recv_row
        table_r[rows, :] = jnp.where(hit, 1.0, 0.0).astype(BF16)
        far = dot(jnp.where(hit, mass_in, 0.0).astype(BF16), ones)
        inv = (STEP_SIZE / scale) / (summed[rows, 3 * LANES:] + far)
        inverse[rows, :] = inv
        for f in range(3):
            lanes = slice(f * LANES, (f + 1) * LANES)
            summed[rows, lanes] = prog[f, rows].astype(F32) + inv * summed[rows, lanes]

    for sem in range(2, 2 + len(SMALL)):
        landing(outgoing, sem)

    def finish(chosen_fields):
        landed = jnp.concatenate([arrived[f].astype(BF16) for f in chosen_fields], axis=1)
        for block_at in range(blocks):
            rows = pl.ds(block_at * ROWS, ROWS)
            far = dot(table_r[rows, :], landed)
            for j, f in enumerate(chosen_fields):
                value = summed[rows, f * LANES:(f + 1) * LANES] + inverse[rows, :] * far[:, j * LANES:(j + 1) * LANES]
                out_hbm[f, rows] = value.astype(out_hbm.dtype)

    finish([2])
    landing(arrived, 1)
    finish([0, 1])
    for sem in range(2):
        landing(outgoing, sem)
    pl.semaphore_wait(mark, 1)


def local(prognostic, metric, coriolis, node_point, send_point, recv_point):
    elements, per, levels = prognostic.shape[1:]
    nodes = elements * per
    sizes = (lax.axis_size("face"), lax.axis_size("sub"))
    groups, slots = link_groups(4 * sizes[1])
    tables, scale = operator_tables()
    links = send_point.shape[0]
    any_spec = pl.BlockSpec(memory_space=pltpu.HBM)
    dma = pltpu.SemaphoreType.DMA
    vmem = pltpu.VMEM
    out = pl.pallas_call(
        functools.partial(kernel, sizes, groups, slots, scale),
        out_shape=pltpu.VMEM((3, nodes, levels), BF16),
        in_specs=[any_spec] * 7,
        out_specs=pl.BlockSpec(memory_space=pltpu.VMEM),
        scratch_shapes=[
            vmem((3, nodes, levels), BF16),
            vmem((4, per, elements), F32),
            vmem((per, elements), F32),
            vmem((per, elements), jnp.int32),
            vmem((1, links), jnp.int32),
            vmem((1, links), jnp.int32),
            vmem((32, BAND), BF16),
            vmem((2, nodes, LANES), F32),
            vmem((4, nodes, LANES), BF16),
            vmem((nodes, 4 * LANES), F32),
            vmem((nodes, LANES), F32),
            vmem((slots, nodes), BF16),
            vmem((nodes, slots), BF16),
            vmem((elements, nodes), BF16),
            vmem((LANES, 3 * LANES), BF16),
            vmem((nodes, LANES), BF16),
            vmem((nodes, LANES), F32),
            vmem((64, nodes), BF16),
            vmem((3, slots, levels), F32),
            vmem((3, slots, levels), F32),
            dma((9,)),
            dma((2 + len(SMALL),)),
            dma((2 + len(SMALL),)),
            pltpu.SemaphoreType.REGULAR((len(groups),)),
            pltpu.SemaphoreType.REGULAR,
        ],
        compiler_params=pltpu.CompilerParams(
            collective_id=0, has_side_effects=True),
    )(
        prognostic.reshape(3, nodes, levels), metric.swapaxes(1, 2), coriolis.T, node_point.T,
        send_point.reshape(1, links), recv_point.reshape(1, links),
        jnp.asarray(tables, dtype=BF16),
    )
    return out.reshape(3, elements, per, levels)


def solution(mesh):
    placed = (
        P(None, ("face", "sub"), None, None),
        P(None, ("face", "sub"), None),
        P(("face", "sub"), None),
        P(("face", "sub"), None),
        P(("face", "sub")),
        P(("face", "sub")),
    )
    return jax.shard_map(
        local,
        mesh=mesh,
        in_specs=placed,
        out_specs=P(None, ("face", "sub"), None, None),
        check_vma=False,
    )
```

```python
import functools
import math

import jax
import jax.numpy as jnp
import numpy as np
from jax import lax
from jax.experimental import pallas as pl
from jax.experimental.pallas import tpu as pltpu
from jax.sharding import PartitionSpec as P

BX = 32
BY = 2
STEP_SIZE = 0.1
ROWS = 256
BAND = 128
LANES = 128
BULK = (2, 3)
SMALL = (0, 1, 4, 5, 6, 7)
LATE = ((2,), (0, 1, 4, 6), (3,), (1, 5, 7))
GREETED = (1, 1, 0, 2, 1, 3, 1, 3)
F32 = jnp.float32
BF16 = jnp.bfloat16
MESH = pl.DeviceIdType.MESH


def gll_tables():
    abscissa = np.array([-1.0, -math.sqrt(0.2), math.sqrt(0.2), 1.0])
    legendre = 0.5 * (5.0 * abscissa * abscissa * abscissa - 3.0 * abscissa)
    derivative = np.zeros((4, 4))
    for target in range(4):
        for source in range(4):
            if target != source:
                derivative[target, source] = legendre[target] / (
                    legendre[source] * (abscissa[target] - abscissa[source])
                )
    derivative[0, 0] = -3.0
    derivative[3, 3] = 3.0
    weights = np.array([1.0, 5.0, 5.0, 1.0]) / 6.0
    return (derivative, weights)


def round_bf16(values):
    return np.asarray(values, dtype=jnp.bfloat16).astype(np.float64)


def operator_tables():
    derivative, weights = gll_tables()
    eye4 = np.eye(4)
    node_weight = np.kron(weights, weights)
    along_c = node_weight[:, None] * np.kron(eye4, derivative)
    along_r = node_weight[:, None] * np.kron(derivative, eye4)
    best = None
    for trial in np.linspace(1.0, 2.0, 2001)[:-1]:
        error = max(
            np.max(np.abs(round_bf16(trial * t) / trial - t) / (np.abs(t).max(1, keepdims=True)))
            for t in (along_c, along_r)
        )
        if best is None or error < best[0]:
            best = (error, trial)
    scale = float(best[1])
    tiles = [np.tile(t, (1, BAND // 16)) for t in (along_c, along_r)]
    stacked = np.concatenate(tiles, axis=0) * scale
    return np.asarray(stacked, dtype=np.float32), scale


def link_groups(lap_blocks):
    side_points = 3 * BY + 1
    top_points = 3 * BX + 1
    group_sizes = [
        (1, side_points),
        (-1, side_points),
        (lap_blocks, top_points),
        (-lap_blocks, top_points),
        (lap_blocks + 1, 1),
        (-lap_blocks - 1, 1),
        (lap_blocks - 1, 1),
        (1 - lap_blocks, 1),
    ]
    starts = [0]
    for _, slot_count in group_sizes:
        starts.append(starts[-1] + slot_count)
    groups = [None] * len(group_sizes)
    first_row = 0
    for k in (0, 1, 2, 4, 3, 5, 6, 7):
        offset, slot_count = group_sizes[k]
        padded = -(-(slot_count + 1) // 8) * 8
        groups[k] = (offset, starts[k], slot_count, first_row, padded)
        first_row += padded
    return groups, first_row


def iota(shape, dim):
    return lax.broadcasted_iota(jnp.int32, shape, dim)


def dot(a, b):
    return lax.dot_general(a, b, (((1,), (0,)), ((), ())), preferred_element_type=F32)


def dot_nt(a, b):
    return lax.dot_general(a, b, (((1,), (1,)), ((), ())), preferred_element_type=F32)


def wait_bytes(ref, sem):
    pltpu.make_async_copy(ref, ref, sem).wait()


def kernel(
    sizes, groups, slots, scale,
    prog_hbm, metric_hbm, cor_hbm, node_hbm, send_hbm, recv_hbm, ops_hbm,
    out_hbm,
    prog, metric, cor, node, sendp, recvp, ops,
    wide, weighted, summed, inverse, table_s, table_r,
    expand, pick, spread, vort, slim,
    outgoing, arrived, in_sem, send_sem, recv_sem, ready, mark,
):
    nface, nsub = sizes
    total = nface * nsub
    nodes = prog.shape[1]
    blocks = nodes // ROWS
    elements = node.shape[1]

    def load(src, dst, k):
        copy = pltpu.make_async_copy(src, dst, in_sem.at[k])
        copy.start()
        return copy

    loads = [load(src, dst, k) for k, (src, dst) in enumerate((
        (metric_hbm, metric), (cor_hbm, cor), (node_hbm, node),
        (send_hbm, sendp), (recv_hbm, recvp), (ops_hbm, ops)))]
    for f in range(3):
        load(prog_hbm.at[f], prog.at[f], 6)

    pl.semaphore_signal(mark, 1)
    me = lax.axis_index("face") * nsub + lax.axis_index("sub")
    lap = 4 * nsub

    def rank(index):
        hops = 4 * (index // lap) + lax.rem(index, lap) // (2 * nsub) + lax.rem(index, nsub)
        return hops * total + index

    peers, lower, first_lap = [], [], []
    for offset, *_ in groups:
        other = lax.rem(me + (offset % total), total)
        peers.append((other // nsub, lax.rem(other, nsub)))
        lower.append(rank(other) < rank(me))
        first_lap.append(other < lap)
    higher = [jnp.logical_not(flag) for flag in lower]
    middle = lower[3] & higher[2]
    turned = me == 0
    later = lax.rem(me // nsub, 2) == 1
    sooner = jnp.logical_not(later)

    barrier = pltpu.get_barrier_semaphore()
    for k, peer in enumerate(peers):
        @pl.when(higher[k])
        def _(peer=peer):
            pl.semaphore_signal(barrier, inc=1, device_id=peer, device_id_type=MESH)
    for _, _, used, first_row, padded in groups:
        gap = pl.ds(first_row + used, padded - used)
        arrived[0:2, gap] = jnp.zeros((2, padded - used, arrived.shape[2]), F32)
        if padded > used + 1:
            gap = pl.ds(first_row + used + 1, padded - used - 1)
            arrived[2:3, gap] = jnp.zeros((1, padded - used - 1, arrived.shape[2]), F32)

    expand[...] = jnp.where(
        iota((elements, nodes), 0) == iota((elements, nodes), 1) >> 4, 1.0, 0.0).astype(BF16)
    pick_l = (iota((LANES, 3 * LANES), 0) & (LANES // 2 - 1)) >> 4
    pick[...] = jnp.where(pick_l == (iota((LANES, 3 * LANES), 1) >> 7), 1.0, 0.0).astype(BF16)
    for copy in loads:
        copy.wait()

    a, b, e, g = metric[0], metric[1], metric[2], metric[3]
    inv_det = 1.0 / (a * g - b * e)
    lane16 = iota((16, 1), 0)
    col, row = lane16 & 3, lane16 >> 2
    w_node = jnp.where((col == 0) | (col == 3), 1 / 6, 5 / 6) * jnp.where((row == 0) | (row == 3), 1 / 6, 5 / 6)
    mass = w_node * inv_det
    parts = [a * inv_det, b * inv_det, e * inv_det, g * inv_det, node[...].astype(F32)]
    stack = jnp.concatenate(parts, axis=0)
    upper = stack.astype(BF16)
    rest = (stack - upper.astype(F32)).astype(BF16)
    spans = dot(jnp.concatenate([upper, rest], axis=0), expand[...])
    half = stack.shape[0]
    spans = spans[:half] + spans[half:]
    own_row = (iota((16, nodes), 1) & 15) == iota((16, nodes), 0)
    row_a, row_b, row_e, row_g, point_row = [
        jnp.sum(jnp.where(own_row, spans[16 * k:16 * k + 16], 0.0), axis=0, keepdims=True) for k in range(5)]

    stack = jnp.concatenate([scale * (mass * cor[...]), mass, parts[4], jnp.zeros_like(mass)], axis=0)
    upper = stack.astype(BF16).astype(F32)
    both = jnp.concatenate([upper, stack - upper], axis=0).T
    own = (iota((16, LANES), 1) & 15) == iota((16, LANES), 0)
    spread[...] = jnp.where(
        own[None], jnp.broadcast_to(both[:, None, :], (elements, 16, LANES)), 0.0
    ).reshape(nodes, LANES).astype(BF16)

    def tile_rows(table):
        return jnp.concatenate([table] * (nodes // BAND), axis=1)

    along_c = tile_rows(ops[0:16, :].astype(F32))
    along_r = tile_rows(ops[16:32, :].astype(F32))
    slim[0:16, :] = (along_c * row_a + along_r * row_e).astype(BF16)
    slim[16:32, :] = (along_c * row_b + along_r * row_g).astype(BF16)
    slim[32:48, :] = (along_c * spans[0:16] + along_r * spans[32:48]).astype(BF16)
    slim[48:64, :] = (along_c * spans[16:32] + along_r * spans[48:64]).astype(BF16)

    count = sendp.shape[1]
    padded = iota((slots, 1), 0)
    slot_of = jnp.full((slots, 1), -1, jnp.int32)
    for _, first_slot, slot_count, first_row, _ in groups:
        inside = (padded >= first_row) & (padded < first_row + slot_count)
        slot_of = jnp.where(inside, padded - first_row + first_slot, slot_of)
    chosen = slot_of == iota((slots, count), 1)
    vacant = jnp.where(slot_of < 0, -1.0, 0.0)
    send_col = jnp.sum(jnp.where(chosen, sendp[...].astype(F32), 0.0), axis=1, keepdims=True) + vacant
    sign = jnp.where(iota((1, nodes), 1) < nodes // 2, 1.0, -1.0)
    table_s[...] = jnp.where(send_col == point_row, sign, 0.0).astype(BF16)

    for part in range(2):
        rows = pl.ds(part * (nodes // 2), nodes // 2)
        first = dot(spread[rows], pick[:, :2 * LANES])
        wide[0, rows] = first[:, :LANES]
        weighted[3, rows] = first[:, LANES:].astype(BF16)

    wait_bytes(prog, in_sem.at[6])

    diagonal = jnp.where(iota((BAND, BAND), 0) >> 4 == iota((BAND, BAND), 1) >> 4, 1.0, 0.0).astype(BF16)

    def block(k, here):
        return jnp.concatenate([slim[k:k + 16, here]] * (BAND // 16), axis=0) * diagonal

    for band in range(nodes // BAND):
        rows = pl.ds(band * BAND, BAND)
        here = pl.ds(band * BAND, BAND)
        left = jnp.concatenate([block(k, here) for k in (0, 16)], axis=1)
        u1, u2, phi = prog[0, rows], prog[1, rows], prog[2, rows]
        right = jnp.concatenate([
            jnp.concatenate([u2, phi * u1], axis=1), jnp.concatenate([-u1, phi * u2], axis=1)], axis=0)
        both_terms = dot(left, right)
        vort[rows, :] = both_terms[:, :LANES]
        weighted[2, rows] = (-both_terms[:, LANES:]).astype(BF16)

    def slot_sum(one, two):
        half = nodes // 2
        terms = [
            dot(table_s[:, h * half:(h + 1) * half],
                jnp.concatenate([weighted[one, pl.ds(h * half, half)], weighted[two, pl.ds(h * half, half)]], axis=1))
            for h in range(2)]
        both_fields = terms[0] - terms[1]
        return both_fields[:, :LANES], both_fields[:, LANES:]

    def copy(k, part, extra, sem):
        rows = pl.ds(groups[k][3], groups[k][2] + extra)
        return pltpu.make_async_remote_copy(
            src_ref=outgoing.at[part, rows], dst_ref=arrived.at[part, rows],
            send_sem=send_sem, recv_sem=recv_sem.at[sem],
            device_id=peers[k], device_id_type=MESH)

    def one_field(k):
        return copy(k, pl.ds(2, 1), 1, 2 if k == 2 else 0)

    def two_fields(k):
        return copy(k, pl.ds(0, 2), 0, 1)

    def early(copies, flag):
        @pl.when(flag)
        def _():
            for item in copies:
                item.start()

    def late(sem, k):
        if k != 1:
            return higher[k]
        return higher[k] & (turned if sem == 3 else jnp.logical_not(turned))

    def answered(sem):
        count = sum(late(sem, k).astype(jnp.int32) for k in LATE[sem])

        @pl.when(count > 0)
        def _():
            pl.semaphore_wait(ready.at[sem], count)

    near_two, slot_mass = slot_sum(2, 3)
    outgoing[2] = near_two
    place = jnp.where(iota((slots, LANES), 1) == (iota((slots, LANES), 0) & (LANES - 1)), slot_mass, 0.0)
    for _, _, used, first_row, size in groups:
        outgoing[2, first_row + used:first_row + used + 1] = jnp.sum(
            place[first_row:first_row + size], axis=0, keepdims=True)
    waited = sum(flag.astype(jnp.int32) for flag in lower)

    @pl.when(waited > 0)
    def _():
        pl.semaphore_wait(barrier, waited)

    early([one_field(2)], lower[2])
    early([one_field(3)], middle)
    for k in SMALL:
        early([one_field(k)], lower[k])
    for k, peer in enumerate(peers):
        other_last = me == total - 1
        for sem, flag in ((GREETED[k ^ 1], lower[k]),) if k else (
                (1, lower[k] & jnp.logical_not(other_last)), (3, lower[k] & other_last)):
            @pl.when(flag)
            def _(peer=peer, sem=sem):
                pl.semaphore_signal(ready.at[sem], inc=1, device_id=peer, device_id_type=MESH)

    for band in range(nodes // BAND):
        rows = pl.ds(band * BAND, BAND)
        here = pl.ds(band * BAND, BAND)
        u1, u2, phi = [prog[f, rows].astype(F32) for f in range(3)]
        energy = (0.5 * (u1 * u1 + u2 * u2) + phi).astype(BF16)
        slopes = dot(jnp.concatenate([block(k, here) for k in (32, 48)], axis=0), energy)
        eta = vort[rows, :] + wide[0, rows]
        weighted[0, rows] = (eta * u2 - slopes[:BAND]).astype(BF16)
        weighted[1, rows] = (-(eta * u1) - slopes[BAND:]).astype(BF16)
    near_zero, near_one = slot_sum(0, 1)
    outgoing[0] = near_zero
    outgoing[1] = near_one
    for k in SMALL:
        early([two_fields(k)], lower[k])
    early([two_fields(2)], lower[2] & sooner)
    early([two_fields(3)], first_lap[3] & lower[3] & sooner)
    recv_col = jnp.sum(jnp.where(chosen, recvp[...].astype(F32), 0.0), axis=1, keepdims=True) + vacant
    same = iota((slots, slots), 0) == iota((slots, slots), 1)
    recv_row = jnp.sum(jnp.where(same, recv_col, 0.0), axis=0, keepdims=True)
    wide[1] = dot(spread[...], pick[:, 2 * LANES:])
    all_weighted = jnp.concatenate([weighted[f] for f in range(4)], axis=1)
    def gather_own(first, last):
        for block_at in range(first, last):
            rows = pl.ds(block_at * ROWS, ROWS)
            point = wide[1, rows][:, 0:1]
            meet = jnp.where(point == point_row, 1.0, 0.0).astype(BF16)
            summed[rows, :] = dot(meet, all_weighted)
            table_r[rows, :] = jnp.where(point == recv_row, 1.0, 0.0).astype(BF16)

    gather_own(0, blocks // 2)
    early([two_fields(2)], lower[2] & later)
    answered(0)
    early([one_field(2)], higher[2])
    answered(1)
    for k in LATE[1]:
        early([one_field(k), two_fields(k)], late(1, k))
    early([two_fields(2)], higher[2])
    gather_own(blocks // 2, blocks)
    early([two_fields(3)], first_lap[3] & lower[3] & later)
    early([one_field(3), two_fields(3)], lower[3] & lower[2])
    answered(2)
    early([one_field(3)], higher[3])
    answered(3)
    for k in LATE[3]:
        early([one_field(k), two_fields(k)], late(3, k))
    early([two_fields(3)], higher[3])

    rows_one = sum(group[2] + 1 for group in groups)
    rows_up = groups[2][2] + 1
    rows_two = sum(group[2] for group in groups)

    def landing(sem):
        wait_bytes((
            arrived.at[pl.ds(2, 1), pl.ds(0, rows_one - rows_up)],
            arrived.at[pl.ds(0, 2), pl.ds(0, rows_two)],
            arrived.at[pl.ds(2, 1), pl.ds(0, rows_up)])[sem], recv_sem.at[sem])

    landing(2)
    early([two_fields(3)], middle & jnp.logical_not(first_lap[3]))
    landing(0)
    sides = [jnp.zeros((1, LANES), F32)] * (slots // LANES)
    for _, _, used, first_row, _ in groups:
        sides[first_row // LANES] += arrived[2, first_row + used:first_row + used + 1]
    mass_in = jnp.concatenate(sides, axis=1)
    ones = jnp.ones((slots, LANES), BF16)
    for block in range(blocks):
        rows = pl.ds(block * ROWS, ROWS)
        far = dot(table_r[rows, :] * mass_in.astype(BF16), ones)
        inv = (STEP_SIZE / scale) / (summed[rows, 3 * LANES:] + far)
        inverse[rows, :] = inv
        for f in range(3):
            lanes = slice(f * LANES, (f + 1) * LANES)
            summed[rows, lanes] = prog[f, rows].astype(F32) + inv * summed[rows, lanes]

    def finish(chosen_fields):
        landed = jnp.concatenate([arrived[f].astype(BF16) for f in chosen_fields], axis=1)
        for block_at in range(blocks):
            rows = pl.ds(block_at * ROWS, ROWS)
            far = dot(table_r[rows, :], landed)
            for j, f in enumerate(chosen_fields):
                value = summed[rows, f * LANES:(f + 1) * LANES] + inverse[rows, :] * far[:, j * LANES:(j + 1) * LANES]
                out_hbm[f, rows] = value.astype(out_hbm.dtype)

    finish([2])
    landing(1)
    finish([0, 1])
    wait_bytes(wide.at[0, pl.ds(0, rows_one + 2 * rows_two)], send_sem)
    pl.semaphore_wait(mark, 1)


def local(prognostic, metric, coriolis, node_point, send_point, recv_point):
    elements, per, levels = prognostic.shape[1:]
    nodes = elements * per
    sizes = (lax.axis_size("face"), lax.axis_size("sub"))
    groups, slots = link_groups(4 * sizes[1])
    tables, scale = operator_tables()
    links = send_point.shape[0]
    any_spec = pl.BlockSpec(memory_space=pltpu.HBM)
    dma = pltpu.SemaphoreType.DMA
    vmem = pltpu.VMEM
    out = pl.pallas_call(
        functools.partial(kernel, sizes, groups, slots, scale),
        out_shape=pltpu.VMEM((3, nodes, levels), BF16),
        in_specs=[any_spec] * 7,
        out_specs=pl.BlockSpec(memory_space=pltpu.VMEM),
        scratch_shapes=[
            vmem((3, nodes, levels), BF16),
            vmem((4, per, elements), F32),
            vmem((per, elements), F32),
            vmem((per, elements), jnp.int32),
            vmem((1, links), jnp.int32),
            vmem((1, links), jnp.int32),
            vmem((32, BAND), BF16),
            vmem((2, nodes, LANES), F32),
            vmem((4, nodes, LANES), BF16),
            vmem((nodes, 4 * LANES), F32),
            vmem((nodes, LANES), F32),
            vmem((slots, nodes), BF16),
            vmem((nodes, slots), BF16),
            vmem((elements, nodes), BF16),
            vmem((LANES, 3 * LANES), BF16),
            vmem((nodes, LANES), BF16),
            vmem((nodes, LANES), F32),
            vmem((64, nodes), BF16),
            vmem((3, slots, levels), F32),
            vmem((3, slots, levels), F32),
            dma((7,)),
            dma,
            dma((3,)),
            pltpu.SemaphoreType.REGULAR((4,)),
            pltpu.SemaphoreType.REGULAR,
        ],
        compiler_params=pltpu.CompilerParams(
            collective_id=0, has_side_effects=True),
    )(
        prognostic.reshape(3, nodes, levels), metric.swapaxes(1, 2), coriolis.T, node_point.T,
        send_point.reshape(1, links), recv_point.reshape(1, links),
        jnp.asarray(tables, dtype=BF16),
    )
    return out.reshape(3, elements, per, levels)


def solution(mesh):
    placed = (
        P(None, ("face", "sub"), None, None),
        P(None, ("face", "sub"), None),
        P(("face", "sub"), None),
        P(("face", "sub"), None),
        P(("face", "sub")),
        P(("face", "sub")),
    )
    return jax.shard_map(
        local,
        mesh=mesh,
        in_specs=placed,
        out_specs=P(None, ("face", "sub"), None, None),
        check_vma=False,
    )
```

```python
import functools
import math

import jax
import jax.numpy as jnp
import numpy as np
from jax import lax
from jax.experimental import pallas as pl
from jax.experimental.pallas import tpu as pltpu
from jax.sharding import PartitionSpec as P

BX = 32
BY = 2
STEP_SIZE = 0.1
ROWS = 256
BAND = 128
LANES = 128
BULK = (2, 3)
SMALL = (0, 1, 4, 5, 6, 7)
LATE = ((2,), (0, 1, 4, 6), (3,), (1, 5, 7))
GREETED = (1, 1, 0, 2, 1, 3, 1, 3)
F32 = jnp.float32
BF16 = jnp.bfloat16
MESH = pl.DeviceIdType.MESH


def gll_tables():
    abscissa = np.array([-1.0, -math.sqrt(0.2), math.sqrt(0.2), 1.0])
    legendre = 0.5 * (5.0 * abscissa * abscissa * abscissa - 3.0 * abscissa)
    derivative = np.zeros((4, 4))
    for target in range(4):
        for source in range(4):
            if target != source:
                derivative[target, source] = legendre[target] / (
                    legendre[source] * (abscissa[target] - abscissa[source])
                )
    derivative[0, 0] = -3.0
    derivative[3, 3] = 3.0
    weights = np.array([1.0, 5.0, 5.0, 1.0]) / 6.0
    return (derivative, weights)


def round_bf16(values):
    return np.asarray(values, dtype=jnp.bfloat16).astype(np.float64)


def operator_tables():
    derivative, weights = gll_tables()
    eye4 = np.eye(4)
    node_weight = np.kron(weights, weights)
    along_c = node_weight[:, None] * np.kron(eye4, derivative)
    along_r = node_weight[:, None] * np.kron(derivative, eye4)
    best = None
    for trial in np.linspace(1.0, 2.0, 2001)[:-1]:
        error = max(
            np.max(np.abs(round_bf16(trial * t) / trial - t) / (np.abs(t).max(1, keepdims=True)))
            for t in (along_c, along_r)
        )
        if best is None or error < best[0]:
            best = (error, trial)
    scale = float(best[1])
    tiles = [np.tile(t, (1, BAND // 16)) for t in (along_c, along_r)]
    stacked = np.concatenate(tiles, axis=0) * scale
    return np.asarray(stacked, dtype=np.float32), scale


def link_groups(lap_blocks):
    side_points = 3 * BY + 1
    top_points = 3 * BX + 1
    group_sizes = [
        (1, side_points),
        (-1, side_points),
        (lap_blocks, top_points),
        (-lap_blocks, top_points),
        (lap_blocks + 1, 1),
        (-lap_blocks - 1, 1),
        (lap_blocks - 1, 1),
        (1 - lap_blocks, 1),
    ]
    starts = [0]
    for _, slot_count in group_sizes:
        starts.append(starts[-1] + slot_count)
    groups = [None] * len(group_sizes)
    first_row = 0
    for k in (0, 1, 2, 4, 3, 5, 6, 7):
        offset, slot_count = group_sizes[k]
        padded = -(-(slot_count + 1) // 8) * 8
        groups[k] = (offset, starts[k], slot_count, first_row, padded)
        first_row += padded
    return groups, first_row


def iota(shape, dim):
    return lax.broadcasted_iota(jnp.int32, shape, dim)


def dot(a, b):
    return lax.dot_general(a, b, (((1,), (0,)), ((), ())), preferred_element_type=F32)


def dot_nt(a, b):
    return lax.dot_general(a, b, (((1,), (1,)), ((), ())), preferred_element_type=F32)


def wait_bytes(ref, sem):
    pltpu.make_async_copy(ref, ref, sem).wait()


def kernel(
    sizes, groups, slots, scale,
    prog_hbm, metric_hbm, cor_hbm, node_hbm, send_hbm, recv_hbm, ops_hbm,
    done, base, inverse, table_r, landed,
    prog, metric, cor, node, sendp, recvp, ops,
    wide, weighted, summed, table_s,
    expand, pick, spread, vort, slim,
    outgoing, arrived, in_sem, send_sem, recv_sem, ready, mark,
):
    nface, nsub = sizes
    total = nface * nsub
    nodes = prog.shape[1]
    blocks = nodes // ROWS
    elements = node.shape[1]

    def load(src, dst, k):
        copy = pltpu.make_async_copy(src, dst, in_sem.at[k])
        copy.start()
        return copy

    loads = [load(src, dst, k) for k, (src, dst) in enumerate((
        (metric_hbm, metric), (cor_hbm, cor), (node_hbm, node),
        (send_hbm, sendp), (recv_hbm, recvp), (ops_hbm, ops)))]
    for f in range(3):
        load(prog_hbm.at[f], prog.at[f], 6)

    pl.semaphore_signal(mark, 1)
    me = lax.axis_index("face") * nsub + lax.axis_index("sub")
    lap = 4 * nsub

    def rank(index):
        hops = 4 * (index // lap) + lax.rem(index, lap) // (2 * nsub) + lax.rem(index, nsub)
        return hops * total + index

    peers, lower, first_lap = [], [], []
    for offset, *_ in groups:
        other = lax.rem(me + (offset % total), total)
        peers.append((other // nsub, lax.rem(other, nsub)))
        lower.append(rank(other) < rank(me))
        first_lap.append(other < lap)
    higher = [jnp.logical_not(flag) for flag in lower]
    middle = lower[3] & higher[2]
    turned = me == 0
    crossing = higher[5] & lower[3]
    later = lax.rem(me // nsub, 2) == 1
    sooner = jnp.logical_not(later)

    barrier = pltpu.get_barrier_semaphore()
    for k, peer in enumerate(peers):
        @pl.when(higher[k])
        def _(peer=peer):
            pl.semaphore_signal(barrier, inc=1, device_id=peer, device_id_type=MESH)
    for _, _, used, first_row, padded in groups:
        gap = pl.ds(first_row + used, padded - used)
        arrived[0:2, gap] = jnp.zeros((2, padded - used, arrived.shape[2]), F32)
        if padded > used + 1:
            gap = pl.ds(first_row + used + 1, padded - used - 1)
            arrived[2:3, gap] = jnp.zeros((1, padded - used - 1, arrived.shape[2]), F32)

    expand[...] = jnp.where(
        iota((elements, nodes), 0) == iota((elements, nodes), 1) >> 4, 1.0, 0.0).astype(BF16)
    pick_l = (iota((LANES, 3 * LANES), 0) & (LANES // 2 - 1)) >> 4
    pick[...] = jnp.where(pick_l == (iota((LANES, 3 * LANES), 1) >> 7), 1.0, 0.0).astype(BF16)
    for copy in loads:
        copy.wait()

    a, b, e, g = metric[0], metric[1], metric[2], metric[3]
    inv_det = 1.0 / (a * g - b * e)
    lane16 = iota((16, 1), 0)
    col, row = lane16 & 3, lane16 >> 2
    w_node = jnp.where((col == 0) | (col == 3), 1 / 6, 5 / 6) * jnp.where((row == 0) | (row == 3), 1 / 6, 5 / 6)
    mass = w_node * inv_det
    parts = [a * inv_det, b * inv_det, e * inv_det, g * inv_det, node[...].astype(F32)]
    stack = jnp.concatenate(parts, axis=0)
    upper = stack.astype(BF16)
    rest = (stack - upper.astype(F32)).astype(BF16)
    spans = dot(jnp.concatenate([upper, rest], axis=0), expand[...])
    half = stack.shape[0]
    spans = spans[:half] + spans[half:]
    own_row = (iota((16, nodes), 1) & 15) == iota((16, nodes), 0)
    row_a, row_b, row_e, row_g, point_row = [
        jnp.sum(jnp.where(own_row, spans[16 * k:16 * k + 16], 0.0), axis=0, keepdims=True) for k in range(5)]

    stack = jnp.concatenate([scale * (mass * cor[...]), mass, parts[4], jnp.zeros_like(mass)], axis=0)
    upper = stack.astype(BF16).astype(F32)
    both = jnp.concatenate([upper, stack - upper], axis=0).T
    own = (iota((16, LANES), 1) & 15) == iota((16, LANES), 0)
    spread[...] = jnp.where(
        own[None], jnp.broadcast_to(both[:, None, :], (elements, 16, LANES)), 0.0
    ).reshape(nodes, LANES).astype(BF16)

    def tile_rows(table):
        return jnp.concatenate([table] * (nodes // BAND), axis=1)

    along_c = tile_rows(ops[0:16, :].astype(F32))
    along_r = tile_rows(ops[16:32, :].astype(F32))
    slim[0:16, :] = (along_c * row_a + along_r * row_e).astype(BF16)
    slim[16:32, :] = (along_c * row_b + along_r * row_g).astype(BF16)
    slim[32:48, :] = (along_c * spans[0:16] + along_r * spans[32:48]).astype(BF16)
    slim[48:64, :] = (along_c * spans[16:32] + along_r * spans[48:64]).astype(BF16)

    count = sendp.shape[1]
    padded = iota((slots, 1), 0)
    slot_of = jnp.full((slots, 1), -1, jnp.int32)
    for _, first_slot, slot_count, first_row, _ in groups:
        inside = (padded >= first_row) & (padded < first_row + slot_count)
        slot_of = jnp.where(inside, padded - first_row + first_slot, slot_of)
    chosen = slot_of == iota((slots, count), 1)
    vacant = jnp.where(slot_of < 0, -1.0, 0.0)
    send_col = jnp.sum(jnp.where(chosen, sendp[...].astype(F32), 0.0), axis=1, keepdims=True) + vacant
    sign = jnp.where(iota((1, nodes), 1) < nodes // 2, 1.0, -1.0)
    table_s[...] = jnp.where(send_col == point_row, sign, 0.0).astype(BF16)

    for part in range(2):
        rows = pl.ds(part * (nodes // 2), nodes // 2)
        first = dot(spread[rows], pick[:, :2 * LANES])
        wide[0, rows] = first[:, :LANES]
        weighted[3, rows] = first[:, LANES:].astype(BF16)

    waited = sum(flag.astype(jnp.int32) for flag in lower)
    prompt = (me == total - 1) | (me == total - lap + 1)

    def enter():
        @pl.when(waited > 0)
        def _():
            pl.semaphore_wait(barrier, waited)

    def reply(flag):
        other_last = me == total - 1
        for k, peer in enumerate(peers):
            for sem, which in ((GREETED[k ^ 1], lower[k]),) if k else (
                    (1, lower[k] & jnp.logical_not(other_last)), (3, lower[k] & other_last)):
                @pl.when(flag & which)
                def _(peer=peer, sem=sem):
                    pl.semaphore_signal(ready.at[sem], inc=1, device_id=peer, device_id_type=MESH)

    @pl.when(prompt)
    def _():
        enter()
        reply(True)

    wait_bytes(prog, in_sem.at[6])

    diagonal = jnp.where(iota((BAND, BAND), 0) >> 4 == iota((BAND, BAND), 1) >> 4, 1.0, 0.0).astype(BF16)

    def block(k, here):
        return jnp.concatenate([slim[k:k + 16, here]] * (BAND // 16), axis=0) * diagonal

    for band in range(nodes // BAND):
        rows = pl.ds(band * BAND, BAND)
        here = pl.ds(band * BAND, BAND)
        left = jnp.concatenate([block(k, here) for k in (0, 16)], axis=1)
        u1, u2, phi = prog[0, rows], prog[1, rows], prog[2, rows]
        right = jnp.concatenate([
            jnp.concatenate([u2, phi * u1], axis=1), jnp.concatenate([-u1, phi * u2], axis=1)], axis=0)
        both_terms = dot(left, right)
        vort[rows, :] = both_terms[:, :LANES]
        weighted[2, rows] = (-both_terms[:, LANES:]).astype(BF16)

    def slot_sum(one, two):
        half = nodes // 2
        terms = [
            dot(table_s[:, h * half:(h + 1) * half],
                jnp.concatenate([weighted[one, pl.ds(h * half, half)], weighted[two, pl.ds(h * half, half)]], axis=1))
            for h in range(2)]
        both_fields = terms[0] - terms[1]
        return both_fields[:, :LANES], both_fields[:, LANES:]

    def copy(k, part, extra, sem):
        rows = pl.ds(groups[k][3], groups[k][2] + extra)
        return pltpu.make_async_remote_copy(
            src_ref=outgoing.at[part, rows], dst_ref=arrived.at[part, rows],
            send_sem=send_sem, recv_sem=recv_sem.at[sem],
            device_id=peers[k], device_id_type=MESH)

    def one_field(k):
        return copy(k, pl.ds(2, 1), 1, 2 if k == 2 else 0)

    def two_fields(k):
        return copy(k, pl.ds(0, 2), 0, 1)

    def early(copies, flag):
        @pl.when(flag)
        def _():
            for item in copies:
                item.start()

    def late(sem, k):
        if k != 1:
            return higher[k]
        return higher[k] & (turned if sem == 3 else jnp.logical_not(turned))

    def answered(sem):
        count = sum(late(sem, k).astype(jnp.int32) for k in LATE[sem])

        @pl.when(count > 0)
        def _():
            pl.semaphore_wait(ready.at[sem], count)

    near_two, slot_mass = slot_sum(2, 3)
    outgoing[2] = near_two
    place = jnp.where(iota((slots, LANES), 1) == (iota((slots, LANES), 0) & (LANES - 1)), slot_mass, 0.0)
    for _, _, used, first_row, size in groups:
        outgoing[2, first_row + used:first_row + used + 1] = jnp.sum(
            place[first_row:first_row + size], axis=0, keepdims=True)
    @pl.when(jnp.logical_not(prompt))
    def _():
        enter()

    early([one_field(2)], lower[2])
    early([one_field(3)], middle)
    for k in SMALL:
        early([one_field(k)], lower[k])
    reply(jnp.logical_not(prompt))

    for band in range(nodes // BAND):
        rows = pl.ds(band * BAND, BAND)
        here = pl.ds(band * BAND, BAND)
        u1, u2, phi = [prog[f, rows].astype(F32) for f in range(3)]
        energy = (0.5 * (u1 * u1 + u2 * u2) + phi).astype(BF16)
        slopes = dot(jnp.concatenate([block(k, here) for k in (32, 48)], axis=0), energy)
        eta = vort[rows, :] + wide[0, rows]
        weighted[0, rows] = (eta * u2 - slopes[:BAND]).astype(BF16)
        weighted[1, rows] = (-(eta * u1) - slopes[BAND:]).astype(BF16)
    near_zero, near_one = slot_sum(0, 1)
    outgoing[0] = near_zero
    outgoing[1] = near_one
    for k in SMALL:
        early([two_fields(k)], lower[k])
    early([two_fields(2)], lower[2] & sooner)
    early([two_fields(3)], first_lap[3] & lower[3] & sooner)
    recv_col = jnp.sum(jnp.where(chosen, recvp[...].astype(F32), 0.0), axis=1, keepdims=True) + vacant
    same = iota((slots, slots), 0) == iota((slots, slots), 1)
    recv_row = jnp.sum(jnp.where(same, recv_col, 0.0), axis=0, keepdims=True)
    wide[1] = dot(spread[...], pick[:, 2 * LANES:])
    all_weighted = jnp.concatenate([weighted[f] for f in range(4)], axis=1)
    def gather_own(first, last):
        for block_at in range(first, last):
            rows = pl.ds(block_at * ROWS, ROWS)
            point = wide[1, rows][:, 0:1]
            meet = jnp.where(point == point_row, 1.0, 0.0).astype(BF16)
            summed[rows, :] = dot(meet, all_weighted)
            table_r[rows, :] = jnp.where(point == recv_row, 1.0, 0.0).astype(BF16)

    gather_own(0, blocks // 2)
    early([two_fields(2)], lower[2] & later)
    answered(0)
    early([one_field(2)], higher[2])
    early([two_fields(2)], higher[2] & higher[3])
    answered(1)
    for k in LATE[1]:
        early([one_field(k), two_fields(k)], late(1, k))
    early([two_fields(2)], higher[2] & lower[3] & jnp.logical_not(crossing))
    gather_own(blocks // 2, blocks)
    early([two_fields(3)], first_lap[3] & lower[3] & later)
    early([one_field(3), two_fields(3)], lower[3] & lower[2])
    answered(2)
    early([one_field(3)], higher[3])
    answered(3)
    for k in LATE[3]:
        early([one_field(k), two_fields(k)], late(3, k))
    early([two_fields(2)], crossing)
    early([two_fields(3)], higher[3] & sooner)

    rows_one = sum(group[2] + 1 for group in groups)
    rows_up = groups[2][2] + 1
    rows_two = sum(group[2] for group in groups)

    def landing(sem):
        wait_bytes((
            arrived.at[pl.ds(2, 1), pl.ds(0, rows_one - rows_up)],
            arrived.at[pl.ds(0, 2), pl.ds(0, rows_two)],
            arrived.at[pl.ds(2, 1), pl.ds(0, rows_up)])[sem], recv_sem.at[sem])

    landing(2)
    early([two_fields(3)], higher[3] & later)
    early([two_fields(3)], middle & jnp.logical_not(first_lap[3]))
    landing(0)
    sides = [jnp.zeros((1, LANES), F32)] * (slots // LANES)
    for _, _, used, first_row, _ in groups:
        sides[first_row // LANES] += arrived[2, first_row + used:first_row + used + 1]
    mass_in = jnp.concatenate(sides, axis=1)
    ones = jnp.ones((slots, LANES), BF16)
    for block in range(blocks):
        rows = pl.ds(block * ROWS, ROWS)
        far = dot(table_r[rows, :] * mass_in.astype(BF16), ones)
        inv = (STEP_SIZE / scale) / (summed[rows, 3 * LANES:] + far)
        inverse[rows, :] = inv
        for f in range(3):
            lanes = slice(f * LANES, (f + 1) * LANES)
            start = prog[f, rows].astype(F32) + inv * summed[rows, lanes]
            if f == 2:
                summed[rows, lanes] = start
            else:
                base[f, rows] = start

    def finish():
        last = arrived[2].astype(BF16)
        for block_at in range(blocks):
            rows = pl.ds(block_at * ROWS, ROWS)
            far = dot(table_r[rows, :], last)
            done[rows, :] = (summed[rows, 2 * LANES:3 * LANES] + inverse[rows, :] * far).astype(BF16)

    finish()
    landing(1)
    for f in range(2):
        landed[f] = arrived[f].astype(BF16)
    wait_bytes(wide.at[0, pl.ds(0, rows_one + 2 * rows_two)], send_sem)
    pl.semaphore_wait(mark, 1)


def closing(done, base, inverse, table_r, landed, out_hbm, fresh, sem):
    nodes = done.shape[0]
    pltpu.make_async_copy(done, out_hbm.at[2], sem).start()
    far_in = jnp.concatenate([landed[0], landed[1]], axis=1)
    for block_at in range(nodes // ROWS):
        rows = pl.ds(block_at * ROWS, ROWS)
        far = dot(table_r[rows, :], far_in)
        for f in range(2):
            fresh[f, rows] = (base[f, rows] + inverse[rows, :] * far[:, f * LANES:(f + 1) * LANES]).astype(BF16)
        pltpu.make_async_copy(fresh.at[:, rows], out_hbm.at[pl.ds(0, 2), rows], sem).start()
    wait_bytes(out_hbm, sem)


def local(prognostic, metric, coriolis, node_point, send_point, recv_point):
    elements, per, levels = prognostic.shape[1:]
    nodes = elements * per
    sizes = (lax.axis_size("face"), lax.axis_size("sub"))
    groups, slots = link_groups(4 * sizes[1])
    tables, scale = operator_tables()
    links = send_point.shape[0]
    any_spec = pl.BlockSpec(memory_space=pltpu.HBM)
    dma = pltpu.SemaphoreType.DMA
    vmem = pltpu.VMEM
    held = pl.pallas_call(
        functools.partial(kernel, sizes, groups, slots, scale),
        out_shape=(
            vmem((nodes, levels), BF16), vmem((2, nodes, levels), F32), vmem((nodes, levels), F32),
            vmem((nodes, slots), BF16), vmem((2, slots, levels), BF16)),
        in_specs=[any_spec] * 7,
        out_specs=[pl.BlockSpec(memory_space=pltpu.VMEM)] * 5,
        scratch_shapes=[
            vmem((3, nodes, levels), BF16),
            vmem((4, per, elements), F32),
            vmem((per, elements), F32),
            vmem((per, elements), jnp.int32),
            vmem((1, links), jnp.int32),
            vmem((1, links), jnp.int32),
            vmem((32, BAND), BF16),
            vmem((2, nodes, LANES), F32),
            vmem((4, nodes, LANES), BF16),
            vmem((nodes, 4 * LANES), F32),
            vmem((slots, nodes), BF16),
            vmem((elements, nodes), BF16),
            vmem((LANES, 3 * LANES), BF16),
            vmem((nodes, LANES), BF16),
            vmem((nodes, LANES), F32),
            vmem((64, nodes), BF16),
            vmem((3, slots, levels), F32),
            vmem((3, slots, levels), F32),
            dma((7,)),
            dma,
            dma((3,)),
            pltpu.SemaphoreType.REGULAR((4,)),
            pltpu.SemaphoreType.REGULAR,
        ],
        compiler_params=pltpu.CompilerParams(
            collective_id=0, has_side_effects=True),
    )(
        prognostic.reshape(3, nodes, levels), metric.swapaxes(1, 2), coriolis.T, node_point.T,
        send_point.reshape(1, links), recv_point.reshape(1, links),
        jnp.asarray(tables, dtype=BF16),
    )
    out = pl.pallas_call(
        closing,
        out_shape=jax.ShapeDtypeStruct((3, nodes, levels), BF16),
        in_specs=[pl.BlockSpec(memory_space=pltpu.VMEM)] * 5,
        out_specs=any_spec,
        scratch_shapes=[vmem((2, nodes, levels), BF16), dma],
        compiler_params=pltpu.CompilerParams(vmem_limit_bytes=8 * 1024 * 1024),
    )(*[pltpu.with_memory_space_constraint(part, pltpu.VMEM) for part in held])
    return out.reshape(3, elements, per, levels)


def solution(mesh):
    placed = (
        P(None, ("face", "sub"), None, None),
        P(None, ("face", "sub"), None),
        P(("face", "sub"), None),
        P(("face", "sub"), None),
        P(("face", "sub")),
        P(("face", "sub")),
    )
    return jax.shard_map(
        local,
        mesh=mesh,
        in_specs=placed,
        out_specs=P(None, ("face", "sub"), None, None),
        check_vma=False,
    )
```

```python
import functools
import math

import jax
import jax.numpy as jnp
import numpy as np
from jax import lax
from jax.experimental import pallas as pl
from jax.experimental.pallas import tpu as pltpu
from jax.sharding import PartitionSpec as P

BX = 32
BY = 2
STEP_SIZE = 0.1
ROWS = 256
BAND = 128
LANES = 128
BULK = (2, 3)
SMALL = (0, 1, 4, 5, 6, 7)
LATE = ((2,), (0, 1, 4, 6), (3,), (1, 5, 7))
GREETED = (1, 1, 0, 2, 1, 3, 1, 3)
F32 = jnp.float32
BF16 = jnp.bfloat16
MESH = pl.DeviceIdType.MESH


def gll_tables():
    abscissa = np.array([-1.0, -math.sqrt(0.2), math.sqrt(0.2), 1.0])
    legendre = 0.5 * (5.0 * abscissa * abscissa * abscissa - 3.0 * abscissa)
    derivative = np.zeros((4, 4))
    for target in range(4):
        for source in range(4):
            if target != source:
                derivative[target, source] = legendre[target] / (
                    legendre[source] * (abscissa[target] - abscissa[source])
                )
    derivative[0, 0] = -3.0
    derivative[3, 3] = 3.0
    weights = np.array([1.0, 5.0, 5.0, 1.0]) / 6.0
    return (derivative, weights)


def round_bf16(values):
    return np.asarray(values, dtype=jnp.bfloat16).astype(np.float64)


def operator_tables():
    derivative, weights = gll_tables()
    eye4 = np.eye(4)
    node_weight = np.kron(weights, weights)
    along_c = node_weight[:, None] * np.kron(eye4, derivative)
    along_r = node_weight[:, None] * np.kron(derivative, eye4)
    best = None
    for trial in np.linspace(1.0, 2.0, 2001)[:-1]:
        error = max(
            np.max(np.abs(round_bf16(trial * t) / trial - t) / (np.abs(t).max(1, keepdims=True)))
            for t in (along_c, along_r)
        )
        if best is None or error < best[0]:
            best = (error, trial)
    scale = float(best[1])
    tiles = [np.tile(t, (1, BAND // 16)) for t in (along_c, along_r)]
    stacked = np.concatenate(tiles, axis=0) * scale
    return np.asarray(stacked, dtype=np.float32), scale


def link_groups(lap_blocks):
    side_points = 3 * BY + 1
    top_points = 3 * BX + 1
    group_sizes = [
        (1, side_points),
        (-1, side_points),
        (lap_blocks, top_points),
        (-lap_blocks, top_points),
        (lap_blocks + 1, 1),
        (-lap_blocks - 1, 1),
        (lap_blocks - 1, 1),
        (1 - lap_blocks, 1),
    ]
    starts = [0]
    for _, slot_count in group_sizes:
        starts.append(starts[-1] + slot_count)
    groups = [None] * len(group_sizes)
    first_row = 0
    for k in (0, 1, 2, 4, 3, 5, 6, 7):
        offset, slot_count = group_sizes[k]
        padded = -(-(slot_count + 1) // 8) * 8
        groups[k] = (offset, starts[k], slot_count, first_row, padded)
        first_row += padded
    return groups, first_row


def iota(shape, dim):
    return lax.broadcasted_iota(jnp.int32, shape, dim)


def dot(a, b):
    return lax.dot_general(a, b, (((1,), (0,)), ((), ())), preferred_element_type=F32)


def dot_nt(a, b):
    return lax.dot_general(a, b, (((1,), (1,)), ((), ())), preferred_element_type=F32)


def wait_bytes(ref, sem):
    pltpu.make_async_copy(ref, ref, sem).wait()


def kernel(
    sizes, groups, slots, scale,
    prog_hbm, metric_hbm, cor_hbm, node_hbm, send_hbm, recv_hbm, ops_hbm,
    done, base, inverse, table_r, landed,
    prog, metric, cor, node, sendp, recvp, ops,
    wide, weighted, summed, table_s,
    expand, pick, spread, vort, slim,
    outgoing, arrived, in_sem, send_sem, recv_sem, ready, mark,
):
    nface, nsub = sizes
    total = nface * nsub
    nodes = prog.shape[1]
    blocks = nodes // ROWS
    elements = node.shape[1]

    def load(src, dst, k):
        copy = pltpu.make_async_copy(src, dst, in_sem.at[k])
        copy.start()
        return copy

    loads = [load(src, dst, k) for k, (src, dst) in enumerate((
        (metric_hbm, metric), (cor_hbm, cor), (node_hbm, node),
        (send_hbm, sendp), (recv_hbm, recvp), (ops_hbm, ops)))]
    for f in range(3):
        load(prog_hbm.at[f], prog.at[f], 6)

    pl.semaphore_signal(mark, 1)
    me = lax.axis_index("face") * nsub + lax.axis_index("sub")
    lap = 4 * nsub

    def rank(index):
        hops = 4 * (index // lap) + lax.rem(index, lap) // (2 * nsub) + lax.rem(index, nsub)
        return hops * total + index

    peers, lower, first_lap = [], [], []
    for offset, *_ in groups:
        other = lax.rem(me + (offset % total), total)
        peers.append((other // nsub, lax.rem(other, nsub)))
        lower.append(rank(other) < rank(me))
        first_lap.append(other < lap)
    higher = [jnp.logical_not(flag) for flag in lower]
    middle = lower[3] & higher[2]
    turned = me == 0
    crossing = higher[5] & lower[3]
    later = lax.rem(me // nsub, 2) == 1
    sooner = jnp.logical_not(later)

    barrier = pltpu.get_barrier_semaphore()
    for k, peer in enumerate(peers):
        @pl.when(higher[k])
        def _(peer=peer):
            pl.semaphore_signal(barrier, inc=1, device_id=peer, device_id_type=MESH)
    for _, _, used, first_row, padded in groups:
        gap = pl.ds(first_row + used, padded - used)
        arrived[0:2, gap] = jnp.zeros((2, padded - used, arrived.shape[2]), F32)
        if padded > used + 1:
            gap = pl.ds(first_row + used + 1, padded - used - 1)
            arrived[2:3, gap] = jnp.zeros((1, padded - used - 1, arrived.shape[2]), F32)

    expand[...] = jnp.where(
        iota((elements, nodes), 0) == iota((elements, nodes), 1) >> 4, 1.0, 0.0).astype(BF16)
    pick_l = (iota((LANES, 3 * LANES), 0) & (LANES // 2 - 1)) >> 4
    pick[...] = jnp.where(pick_l == (iota((LANES, 3 * LANES), 1) >> 7), 1.0, 0.0).astype(BF16)
    for copy in loads:
        copy.wait()

    a, b, e, g = metric[0], metric[1], metric[2], metric[3]
    inv_det = 1.0 / (a * g - b * e)
    lane16 = iota((16, 1), 0)
    col, row = lane16 & 3, lane16 >> 2
    w_node = jnp.where((col == 0) | (col == 3), 1 / 6, 5 / 6) * jnp.where((row == 0) | (row == 3), 1 / 6, 5 / 6)
    mass = w_node * inv_det
    parts = [a * inv_det, b * inv_det, e * inv_det, g * inv_det, node[...].astype(F32)]
    stack = jnp.concatenate(parts, axis=0)
    upper = stack.astype(BF16)
    rest = (stack - upper.astype(F32)).astype(BF16)
    spans = dot(jnp.concatenate([upper, rest], axis=0), expand[...])
    half = stack.shape[0]
    spans = spans[:half] + spans[half:]
    own_row = (iota((16, nodes), 1) & 15) == iota((16, nodes), 0)
    row_a, row_b, row_e, row_g, point_row = [
        jnp.sum(jnp.where(own_row, spans[16 * k:16 * k + 16], 0.0), axis=0, keepdims=True) for k in range(5)]

    stack = jnp.concatenate([scale * (mass * cor[...]), mass, parts[4], jnp.zeros_like(mass)], axis=0)
    upper = stack.astype(BF16).astype(F32)
    both = jnp.concatenate([upper, stack - upper], axis=0).T
    own = (iota((16, LANES), 1) & 15) == iota((16, LANES), 0)
    spread[...] = jnp.where(
        own[None], jnp.broadcast_to(both[:, None, :], (elements, 16, LANES)), 0.0
    ).reshape(nodes, LANES).astype(BF16)

    def tile_rows(table):
        return jnp.concatenate([table] * (nodes // BAND), axis=1)

    along_c = tile_rows(ops[0:16, :].astype(F32))
    along_r = tile_rows(ops[16:32, :].astype(F32))
    slim[0:16, :] = (along_c * row_a + along_r * row_e).astype(BF16)
    slim[16:32, :] = (along_c * row_b + along_r * row_g).astype(BF16)
    slim[32:48, :] = (along_c * spans[0:16] + along_r * spans[32:48]).astype(BF16)
    slim[48:64, :] = (along_c * spans[16:32] + along_r * spans[48:64]).astype(BF16)

    count = sendp.shape[1]
    padded = iota((slots, 1), 0)
    slot_of = jnp.full((slots, 1), -1, jnp.int32)
    for _, first_slot, slot_count, first_row, _ in groups:
        inside = (padded >= first_row) & (padded < first_row + slot_count)
        slot_of = jnp.where(inside, padded - first_row + first_slot, slot_of)
    chosen = slot_of == iota((slots, count), 1)
    vacant = jnp.where(slot_of < 0, -1.0, 0.0)
    send_col = jnp.sum(jnp.where(chosen, sendp[...].astype(F32), 0.0), axis=1, keepdims=True) + vacant
    sign = jnp.where(iota((1, nodes), 1) < nodes // 2, 1.0, -1.0)
    table_s[...] = jnp.where(send_col == point_row, sign, 0.0).astype(BF16)

    for part in range(2):
        rows = pl.ds(part * (nodes // 2), nodes // 2)
        first = dot(spread[rows], pick[:, :2 * LANES])
        wide[0, rows] = first[:, :LANES]
        weighted[3, rows] = first[:, LANES:].astype(BF16)

    waited = sum(flag.astype(jnp.int32) for flag in lower)
    prompt = (me == total - 1) | (me == total - lap + 1)

    def enter():
        @pl.when(waited > 0)
        def _():
            pl.semaphore_wait(barrier, waited)

    def reply(flag):
        other_last = me == total - 1
        for k, peer in enumerate(peers):
            for sem, which in ((GREETED[k ^ 1], lower[k]),) if k else (
                    (1, lower[k] & jnp.logical_not(other_last)), (3, lower[k] & other_last)):
                @pl.when(flag & which)
                def _(peer=peer, sem=sem):
                    pl.semaphore_signal(ready.at[sem], inc=1, device_id=peer, device_id_type=MESH)

    @pl.when(prompt)
    def _():
        enter()
        reply(True)

    wait_bytes(prog, in_sem.at[6])

    diagonal = jnp.where(iota((BAND, BAND), 0) >> 4 == iota((BAND, BAND), 1) >> 4, 1.0, 0.0).astype(BF16)

    def block(k, here):
        return jnp.concatenate([slim[k:k + 16, here]] * (BAND // 16), axis=0) * diagonal

    for band in range(nodes // BAND):
        rows = pl.ds(band * BAND, BAND)
        here = pl.ds(band * BAND, BAND)
        left = jnp.concatenate([block(k, here) for k in (0, 16)], axis=1)
        u1, u2, phi = prog[0, rows], prog[1, rows], prog[2, rows]
        right = jnp.concatenate([
            jnp.concatenate([u2, phi * u1], axis=1), jnp.concatenate([-u1, phi * u2], axis=1)], axis=0)
        both_terms = dot(left, right)
        vort[rows, :] = both_terms[:, :LANES]
        weighted[2, rows] = (-both_terms[:, LANES:]).astype(BF16)

    def slot_sum(one, two):
        half = nodes // 2
        terms = [
            dot(table_s[:, h * half:(h + 1) * half],
                jnp.concatenate([weighted[one, pl.ds(h * half, half)], weighted[two, pl.ds(h * half, half)]], axis=1))
            for h in range(2)]
        both_fields = terms[0] - terms[1]
        return both_fields[:, :LANES], both_fields[:, LANES:]

    def copy(k, part, extra, sem):
        rows = pl.ds(groups[k][3], groups[k][2] + extra)
        return pltpu.make_async_remote_copy(
            src_ref=outgoing.at[part, rows], dst_ref=arrived.at[part, rows],
            send_sem=send_sem, recv_sem=recv_sem.at[sem],
            device_id=peers[k], device_id_type=MESH)

    def one_field(k):
        return copy(k, pl.ds(2, 1), 1, 2 if k == 2 else 0)

    def two_fields(k):
        return copy(k, pl.ds(0, 2), 0, 1)

    def early(copies, flag):
        @pl.when(flag)
        def _():
            for item in copies:
                item.start()

    def late(sem, k):
        if k != 1:
            return higher[k]
        return higher[k] & (turned if sem == 3 else jnp.logical_not(turned))

    def answered(sem):
        count = sum(late(sem, k).astype(jnp.int32) for k in LATE[sem])

        @pl.when(count > 0)
        def _():
            pl.semaphore_wait(ready.at[sem], count)

    near_two, slot_mass = slot_sum(2, 3)
    outgoing[2] = near_two
    place = jnp.where(iota((slots, LANES), 1) == (iota((slots, LANES), 0) & (LANES - 1)), slot_mass, 0.0)
    for _, _, used, first_row, size in groups:
        outgoing[2, first_row + used:first_row + used + 1] = jnp.sum(
            place[first_row:first_row + size], axis=0, keepdims=True)
    @pl.when(jnp.logical_not(prompt))
    def _():
        enter()

    early([one_field(2)], lower[2])
    early([one_field(3)], middle)
    for k in SMALL:
        early([one_field(k)], lower[k])
    reply(jnp.logical_not(prompt))

    for band in range(nodes // BAND):
        rows = pl.ds(band * BAND, BAND)
        here = pl.ds(band * BAND, BAND)
        u1, u2, phi = [prog[f, rows].astype(F32) for f in range(3)]
        energy = (0.5 * (u1 * u1 + u2 * u2) + phi).astype(BF16)
        slopes = dot(jnp.concatenate([block(k, here) for k in (32, 48)], axis=0), energy)
        eta = vort[rows, :] + wide[0, rows]
        weighted[0, rows] = (eta * u2 - slopes[:BAND]).astype(BF16)
        weighted[1, rows] = (-(eta * u1) - slopes[BAND:]).astype(BF16)
    near_zero, near_one = slot_sum(0, 1)
    outgoing[0] = near_zero
    outgoing[1] = near_one
    for k in SMALL:
        early([two_fields(k)], lower[k])
    early([two_fields(2)], lower[2] & sooner)
    early([two_fields(3)], first_lap[3] & lower[3] & sooner)
    recv_col = jnp.sum(jnp.where(chosen, recvp[...].astype(F32), 0.0), axis=1, keepdims=True) + vacant
    same = iota((slots, slots), 0) == iota((slots, slots), 1)
    recv_row = jnp.sum(jnp.where(same, recv_col, 0.0), axis=0, keepdims=True)
    wide[1] = dot(spread[...], pick[:, 2 * LANES:])
    all_weighted = jnp.concatenate([weighted[f] for f in range(4)], axis=1)
    def gather_own(first, last):
        for block_at in range(first, last):
            rows = pl.ds(block_at * ROWS, ROWS)
            point = wide[1, rows][:, 0:1]
            meet = jnp.where(point == point_row, 1.0, 0.0).astype(BF16)
            summed[rows, :] = dot(meet, all_weighted)
            table_r[rows, :] = jnp.where(point == recv_row, 1.0, 0.0).astype(BF16)

    gather_own(0, blocks // 2)
    early([two_fields(2)], lower[2] & later)
    answered(0)
    early([one_field(2)], higher[2])
    early([two_fields(2)], higher[2] & higher[3])
    answered(1)
    for k in LATE[1]:
        early([one_field(k), two_fields(k)], late(1, k))
    early([two_fields(2)], higher[2] & lower[3] & jnp.logical_not(crossing))
    gather_own(blocks // 2, blocks)
    early([two_fields(3)], first_lap[3] & lower[3] & later)
    early([one_field(3), two_fields(3)], lower[3] & lower[2])
    answered(2)
    early([one_field(3)], higher[3])
    answered(3)
    for k in LATE[3]:
        early([one_field(k), two_fields(k)], late(3, k))
    early([two_fields(2)], crossing)
    early([two_fields(3)], higher[3] & sooner)

    rows_one = sum(group[2] + 1 for group in groups)
    rows_up = groups[2][2] + 1
    rows_two = sum(group[2] for group in groups)

    def landing(sem):
        wait_bytes((
            arrived.at[pl.ds(2, 1), pl.ds(0, rows_one - rows_up)],
            arrived.at[pl.ds(0, 2), pl.ds(0, rows_two)],
            arrived.at[pl.ds(2, 1), pl.ds(0, rows_up)])[sem], recv_sem.at[sem])

    landing(2)
    early([two_fields(3)], higher[3] & later)
    early([two_fields(3)], middle & jnp.logical_not(first_lap[3]))
    landing(0)
    sides = [jnp.zeros((1, LANES), F32)] * (slots // LANES)
    for _, _, used, first_row, _ in groups:
        sides[first_row // LANES] += arrived[2, first_row + used:first_row + used + 1]
    mass_in = jnp.concatenate(sides, axis=1)
    ones = jnp.ones((slots, LANES), BF16)
    for block in range(blocks):
        rows = pl.ds(block * ROWS, ROWS)
        far = dot(table_r[rows, :] * mass_in.astype(BF16), ones)
        inv = (STEP_SIZE / scale) / (summed[rows, 3 * LANES:] + far)
        inverse[rows, :] = inv
        for f in range(3):
            lanes = slice(f * LANES, (f + 1) * LANES)
            start = prog[f, rows].astype(F32) + inv * summed[rows, lanes]
            if f == 2:
                summed[rows, lanes] = start
            else:
                base[f, rows] = start

    def finish():
        last = arrived[2].astype(BF16)
        for block_at in range(blocks):
            rows = pl.ds(block_at * ROWS, ROWS)
            far = dot(table_r[rows, :], last)
            done[rows, :] = (summed[rows, 2 * LANES:3 * LANES] + inverse[rows, :] * far).astype(BF16)

    finish()
    landing(1)
    for f in range(2):
        landed[f] = arrived[f].astype(BF16)
    wait_bytes(wide.at[0, pl.ds(0, rows_one + 2 * rows_two)], send_sem)
    pl.semaphore_wait(mark, 1)


def closing(done, base, inverse, table_r, landed, out_hbm, fresh, sem):
    nodes = done.shape[0]
    pltpu.make_async_copy(done, out_hbm.at[2], sem).start()
    far_in = jnp.concatenate([landed[0], landed[1]], axis=1)
    for block_at in range(nodes // BAND):
        rows = pl.ds(block_at * BAND, BAND)
        far = dot(table_r[rows, :], far_in)
        for f in range(2):
            fresh[f, rows] = (base[f, rows] + inverse[rows, :] * far[:, f * LANES:(f + 1) * LANES]).astype(BF16)
        pltpu.make_async_copy(fresh.at[:, rows], out_hbm.at[pl.ds(0, 2), rows], sem).start()
    wait_bytes(out_hbm, sem)


def local(prognostic, metric, coriolis, node_point, send_point, recv_point):
    elements, per, levels = prognostic.shape[1:]
    nodes = elements * per
    sizes = (lax.axis_size("face"), lax.axis_size("sub"))
    groups, slots = link_groups(4 * sizes[1])
    tables, scale = operator_tables()
    links = send_point.shape[0]
    any_spec = pl.BlockSpec(memory_space=pltpu.HBM)
    dma = pltpu.SemaphoreType.DMA
    vmem = pltpu.VMEM
    held = pl.pallas_call(
        functools.partial(kernel, sizes, groups, slots, scale),
        out_shape=(
            vmem((nodes, levels), BF16), vmem((2, nodes, levels), F32), vmem((nodes, levels), F32),
            vmem((nodes, slots), BF16), vmem((2, slots, levels), BF16)),
        in_specs=[any_spec] * 7,
        out_specs=[pl.BlockSpec(memory_space=pltpu.VMEM)] * 5,
        scratch_shapes=[
            vmem((3, nodes, levels), BF16),
            vmem((4, per, elements), F32),
            vmem((per, elements), F32),
            vmem((per, elements), jnp.int32),
            vmem((1, links), jnp.int32),
            vmem((1, links), jnp.int32),
            vmem((32, BAND), BF16),
            vmem((2, nodes, LANES), F32),
            vmem((4, nodes, LANES), BF16),
            vmem((nodes, 4 * LANES), F32),
            vmem((slots, nodes), BF16),
            vmem((elements, nodes), BF16),
            vmem((LANES, 3 * LANES), BF16),
            vmem((nodes, LANES), BF16),
            vmem((nodes, LANES), F32),
            vmem((64, nodes), BF16),
            vmem((3, slots, levels), F32),
            vmem((3, slots, levels), F32),
            dma((7,)),
            dma,
            dma((3,)),
            pltpu.SemaphoreType.REGULAR((4,)),
            pltpu.SemaphoreType.REGULAR,
        ],
        compiler_params=pltpu.CompilerParams(
            collective_id=0, has_side_effects=True),
    )(
        prognostic.reshape(3, nodes, levels), metric.swapaxes(1, 2), coriolis.T, node_point.T,
        send_point.reshape(1, links), recv_point.reshape(1, links),
        jnp.asarray(tables, dtype=BF16),
    )
    out = pl.pallas_call(
        closing,
        out_shape=jax.ShapeDtypeStruct((3, nodes, levels), BF16),
        in_specs=[pl.BlockSpec(memory_space=pltpu.VMEM)] * 5,
        out_specs=any_spec,
        scratch_shapes=[vmem((2, nodes, levels), BF16), dma],
        compiler_params=pltpu.CompilerParams(vmem_limit_bytes=8 * 1024 * 1024),
    )(*[pltpu.with_memory_space_constraint(part, pltpu.VMEM) for part in held])
    return out.reshape(3, elements, per, levels)


def solution(mesh):
    placed = (
        P(None, ("face", "sub"), None, None),
        P(None, ("face", "sub"), None),
        P(("face", "sub"), None),
        P(("face", "sub"), None),
        P(("face", "sub")),
        P(("face", "sub")),
    )
    return jax.shard_map(
        local,
        mesh=mesh,
        in_specs=placed,
        out_specs=P(None, ("face", "sub"), None, None),
        check_vma=False,
    )
```
